32 devices in a mesh: gx: 8 (over y, x, core), gy: 4 (over z).
Axes of the slice: x: 2, y: 2, z: 4, core: 2. Of those that a mesh axis runs over, the one named last changes fastest.
Arguments:
- source_field: bfloat16 [4096, 128, 128], P(('gx', 'gy')), may hold values from -6 to 6
- weight_blocks: bfloat16 [16384, 128, 128], P(('gx', 'gy')), may hold values from -0.1875 to 0.1875
- source_ids: int32 [16384], replicated, may hold values from 0 to 4095, as said below
- target_ids: int32 [16384], replicated, may hold values from 0 to 2047, as said below
Outputs:
- remapped: bfloat16 [2048, 128, 128], P(('gx', 'gy'))
The draws below stay inside these ranges and needn't reach their ends.
Inputs may be any that keep to these rules, and one draw needn't show every extreme that they name: `source_ids`: source block b lies on device b // 128 of gx+gy, and weight block k lies on device k // 512. The weight blocks of device d name only source blocks of devices d - 2 to d + 2. Among the weight blocks of one device, at most 64 distinct source blocks of any one other device are named, and exactly 64 for some other device. `target_ids`: target block t lies on device t // 64 of gx+gy. The weight blocks of device d name only target blocks of devices d - 2 to d + 2. Among the weight blocks of one device, at most 16 distinct target blocks of any one device are named, and exactly 16 for some other device.
All inputs are finite; a program needn't handle non-finite values.
Results may differ from the reference program's by a relative error of at most 0.001.
Values may be sent and summed in bfloat16 or wider, within the bound.
A program may use at most 192 MiB of HBM per device.

```python
import jax
import jax.numpy as jnp
from jax import lax

BLK = 128
CH = 128
HALF = 2
SB_DEV = 128
TB_DEV = 64
WB_DEV = 512
CAP_S = 64
CAP_T = 16
NSB = 4096
NW = 16384
N_GX = 8
N_GY = 4


def pair_ids(key, slot_count, per_device):
    devices = N_GX * N_GY
    span = 2 * HALF + 1

    def one_device(device):
        keyed = jax.random.fold_in(key, device)
        key_count, key_force, key_perm, key_pick, key_order = jax.random.split(keyed, 5)
        offsets = jnp.arange(span, dtype=jnp.int32) - HALF
        owner = device + offsets
        valid = (owner >= 0) & (owner < devices)
        counts = jax.random.randint(key_count, (span,), slot_count // 2, slot_count + 1)
        scores = jax.random.randint(key_force, (span,), 0, 1024) * span + jnp.arange(span, dtype=jnp.int32)
        scores = jnp.where(valid & (offsets != 0), scores, -1)
        forced = jnp.argmax(scores)
        counts = jnp.where((jnp.arange(span, dtype=jnp.int32) == forced) | (offsets == 0), slot_count, counts)
        counts = jnp.where(valid, counts, 0)
        perms = jax.vmap(lambda kk: jax.random.permutation(kk, per_device))(jax.random.split(key_perm, span))
        chosen = perms[:, :slot_count].reshape(-1)
        used = (jnp.arange(slot_count, dtype=jnp.int32)[None, :] < counts[:, None]).reshape(-1)
        entries = span * slot_count
        block_index = jnp.arange(WB_DEV, dtype=jnp.int32)
        picked = jax.random.randint(key_pick, (WB_DEV,), 0, entries)
        entry = jnp.where(block_index < entries, block_index, picked)
        entry = jnp.where(used[entry], entry, HALF * slot_count + entry % slot_count)
        order = jax.random.permutation(key_order, WB_DEV)
        entry = entry[order]
        return (owner[entry // slot_count] * per_device + chosen[entry]).astype(jnp.int32)
    return jax.vmap(one_device)(jnp.arange(devices, dtype=jnp.int32)).reshape(-1).astype(jnp.int32)


def draw_source_ids(key, part):
    return pair_ids(jax.random.fold_in(key, 11), CAP_S, SB_DEV)


def draw_target_ids(key, part):
    return pair_ids(jax.random.fold_in(key, 23), CAP_T, TB_DEV)


def shard_levels(stream_key, shape, pieces, least, largest):
    gain = 1.0
    for dim, parts in pieces:
        draws = jax.random.uniform(jax.random.fold_in(jax.random.fold_in(stream_key, 6), dim), (parts,), jnp.float32, least / len(pieces), largest / len(pieces))
        gain = gain * jnp.repeat(jnp.exp(draws), shape[dim] // parts).reshape((-1,) + (1,) * (len(shape) - 1 - dim))
    return gain


def centred(own_key, shape, scale, most, cuts=(), kind=jnp.bfloat16):
    gain = shard_levels(own_key, shape, cuts, -0.22, 0.18) if cuts else 1.0
    array = jax.random.normal(own_key, shape, jnp.float32) * scale * gain
    return jnp.minimum(jnp.maximum(array, -most), most).astype(kind)


def setup_inputs(seed: int = 0) -> dict:
    splits = jax.random.split(jax.random.key(seed), 5)
    return {
        "source_field": centred(splits[0], (NSB, BLK, CH), 1.0, 6.0, ((0, 32),)),
        "weight_blocks": centred(splits[1], (NW, BLK, BLK), (BLK * WB_DEV // TB_DEV) ** -0.5, 0.1875, ((0, 32),)),
        "source_ids": draw_source_ids(jax.random.fold_in(splits[4], 71), 0),
        "target_ids": draw_target_ids(jax.random.fold_in(splits[4], 71), 0),
    }


def reference(source_field, weight_blocks, source_ids, target_ids):
    devices = N_GX * N_GY
    total = jnp.zeros((TB_DEV * devices, BLK, CH), jnp.float32)

    def accumulate(carry, index):
        start = (index * WB_DEV).astype(jnp.int32)
        weights = lax.dynamic_slice_in_dim(weight_blocks, start, WB_DEV, 0)
        src_rows = lax.dynamic_slice_in_dim(source_ids, start, WB_DEV, 0)
        tgt_rows = lax.dynamic_slice_in_dim(target_ids, start, WB_DEV, 0)
        gathered = source_field[src_rows]
        partial_value = jnp.einsum("kts,ksc->ktc", weights.astype(jnp.float32), gathered.astype(jnp.float32))
        return carry.at[tgt_rows].add(partial_value), None

    total, _ = lax.scan(accumulate, total, jnp.arange(devices, dtype=jnp.int32))
    return total.astype(jnp.bfloat16)
```

```python
import functools

import jax
import jax.numpy as jnp
from jax import lax
from jax.experimental import pallas as pl
from jax.experimental.pallas import tpu as pltpu
from jax.sharding import PartitionSpec as P

HALF = 2
TB_DEV = 64
CAP_S = 64
CAP_T = 16
SPAN = 2 * HALF + 1
AXES = ("gx", "gy")
ARRIVALS = (-2, 2, -1, 1)
STAGES = (0,) + ARRIVALS
DEPTH = 32
UNROLL = 4
LOW_EXPONENT = -110.0


def passed_along(value, steps):
    count = lax.axis_size(AXES)
    initial, last = (max(0, -steps), min(count, count - steps))
    return lax.ppermute(value, AXES, [(source, source + steps) for source in range(initial, last)])


def rows_of(ids, device, devices, held):
    clamped = jnp.clip(device, 0, devices - 1)
    return lax.dynamic_slice_in_dim(ids, clamped * held, held, 0)


def named(rows, low, count):
    return jnp.any(rows[:, None] == low + jnp.arange(count, dtype=jnp.int32)[None, :], axis=0)


def ranks_of(asked):
    count = asked.shape[1]
    before = jnp.arange(count)[:, None] < jnp.arange(count)[None, :]
    return jnp.sum((asked[:, :, None] & before[None]).astype(jnp.int32), axis=1)


def stage_kernel(stage, last, *refs):
    bounds, packed, w_hbm, src = refs[:4]
    refs = refs[4:]
    if stage > 0:
        acc_in, refs = refs[0], refs[1:]
    if last:
        outs, acc, wbuf, sems = refs[:SPAN], refs[SPAN], refs[SPAN + 1], refs[SPAN + 2]
    else:
        acc, wbuf, sems = refs
    first = bounds[stage]
    total = bounds[stage + 1] - first

    def copy_of(i):
        slot = lax.rem(i, DEPTH)
        k = packed[first + i] // (256 * 128)
        return pltpu.make_async_copy(w_hbm.at[k], wbuf.at[slot], sems.at[slot])

    def issue(i, carry):
        copy_of(i).start()
        return carry

    lax.fori_loop(0, jnp.minimum(total, DEPTH), issue, 0)
    if stage > 0:
        acc[...] = acc_in[...]
    else:
        acc[...] = jnp.zeros_like(acc)

    def run(begin, width):
        sums = []
        for u in range(width):
            i = begin + u
            copy_of(i).wait()
            s = (packed[first + i] // 128) % 256
            sums.append(
                jnp.dot(wbuf[lax.rem(i, DEPTH)], src[s], preferred_element_type=jnp.float32)
            )
        for u in range(width):
            t = packed[first + begin + u] % 128
            acc[t] += sums[u]
        for u in range(width):
            i = begin + u + DEPTH

            @pl.when(i < total)
            def _():
                copy_of(i).start()

    def wide(g, carry):
        run(g * UNROLL, UNROLL)
        return carry

    def narrow(i, carry):
        run(i, 1)
        return carry

    groups = total // UNROLL
    lax.fori_loop(0, groups, wide, 0)
    lax.fori_loop(groups * UNROLL, total, narrow, 0)

    if last:
        for r in range(SPAN):
            if r == HALF:
                outs[r][...] = acc[r * CAP_T : (r + 1) * CAP_T]
                continue
            rows = lax.broadcasted_iota(jnp.int32, acc.shape[1:], 0)

            def encode(b, exponents, r=r):
                value = acc[r * CAP_T + b]
                most = jnp.max(jnp.abs(value), axis=0, keepdims=True)
                exponent = jnp.ceil(jnp.log(jnp.maximum(most, 1e-37)) * 1.4426950408889634)
                exponent = jnp.maximum(exponent, LOW_EXPONENT)
                scaled = jnp.floor(value * jnp.exp2(15.0 - exponent) + 0.5)
                scaled = jnp.clip(scaled, -32767.0, 32767.0)
                outs[r][b] = scaled.astype(jnp.int32).astype(jnp.int16)
                return jnp.where(rows == b, exponent.astype(jnp.int32), exponents)

            exponents = lax.fori_loop(0, CAP_T, encode, jnp.zeros(acc.shape[1:], jnp.int32))
            outs[r][CAP_T] = exponents.astype(jnp.int16)


def stage_call(stage, bounds, packed, weights, src, acc):
    last = stage == SPAN - 1
    tile = weights.shape[1:2] + src.shape[2:]
    acc_shape = (SPAN * CAP_T,) + tile
    smem = pl.BlockSpec(memory_space=pltpu.SMEM)
    vmem = pl.BlockSpec(memory_space=pltpu.VMEM)
    args = [bounds, packed, weights, src] + ([acc] if stage > 0 else [])
    in_specs = [smem, smem, pl.BlockSpec(memory_space=pl.ANY), vmem] + ([vmem] if stage > 0 else [])
    buffers = [
        pltpu.VMEM((DEPTH,) + weights.shape[1:], weights.dtype),
        pltpu.SemaphoreType.DMA((DEPTH,)),
    ]
    if last:
        out_shape = [
            jax.ShapeDtypeStruct((CAP_T,) + tile, jnp.float32)
            if r == HALF
            else jax.ShapeDtypeStruct((CAP_T + 1,) + tile, jnp.int16)
            for r in range(SPAN)
        ]
        out_specs = [vmem] * SPAN
        buffers = [pltpu.VMEM(acc_shape, jnp.float32)] + buffers
    else:
        out_shape = jax.ShapeDtypeStruct(acc_shape, jnp.float32)
        out_specs = vmem
    share = weights.shape[0] // SPAN
    return pl.pallas_call(
        functools.partial(stage_kernel, stage, last),
        out_shape=out_shape,
        in_specs=in_specs,
        out_specs=out_specs,
        scratch_shapes=buffers,
        name=f"stage_{stage}",
        cost_estimate=pl.CostEstimate(
            flops=share * 2 * 128**3, bytes_accessed=24 * 2**20, transcendentals=0
        ),
        compiler_params=pltpu.CompilerParams(vmem_limit_bytes=40 * 2**20),
    )(*args)


def final_kernel(places, *refs):
    boxes, out = refs[:SPAN], refs[SPAN]
    scales = refs[SPAN + 1]
    for s in range(SPAN):
        if s != HALF:
            scales[s] = jnp.exp2(boxes[s][CAP_T].astype(jnp.float32) - 15.0)[:CAP_T]

    def one(b, carry):
        total = jnp.zeros(out.shape[1:], jnp.float32)
        for s in range(SPAN):
            place = places[s * TB_DEV + b]
            slot = jnp.maximum(place, 0)
            if s == HALF:
                value = boxes[s][slot]
            else:
                value = boxes[s][slot].astype(jnp.float32) * scales[s, pl.ds(slot, 1), :]
            total = total + jnp.where(place >= 0, value, 0.0)
        out[b] = total.astype(out.dtype)
        return carry

    lax.fori_loop(0, TB_DEV, one, 0)


def final_call(places, boxes):
    tile = boxes[HALF].shape[1:]
    vmem = pl.BlockSpec(memory_space=pltpu.VMEM)
    return pl.pallas_call(
        final_kernel,
        out_shape=jax.ShapeDtypeStruct((TB_DEV,) + tile, jnp.bfloat16),
        in_specs=[pl.BlockSpec(memory_space=pltpu.SMEM)] + [vmem] * SPAN,
        out_specs=vmem,
        scratch_shapes=[pltpu.VMEM((SPAN, CAP_T, tile[1]), jnp.float32)],
        name="final_sum",
        compiler_params=pltpu.CompilerParams(vmem_limit_bytes=32 * 2**20),
    )(places, *boxes)


def body(source_field, weight_blocks, source_ids, target_ids):
    devices = lax.axis_size(AXES)
    myself = lax.axis_index(AXES)
    held = weight_blocks.shape[0]
    src_count = source_field.shape[0]

    asked = jnp.stack(
        [
            named(rows_of(source_ids, myself - rel, devices, held), myself * src_count, src_count)
            for rel in ARRIVALS
        ]
    )
    ranks = ranks_of(asked)
    matches = asked[:, None, :] & (
        ranks[:, None, :] == jnp.arange(CAP_S, dtype=jnp.int32)[None, :, None]
    )
    chosen = jnp.sum(
        jnp.where(matches, jnp.arange(src_count, dtype=jnp.int32)[None, None, :], 0), axis=2
    )
    arrived = []
    for n, rel in enumerate(ARRIVALS):
        arrived.append(passed_along(source_field[chosen[n]], -rel))

    own_src = rows_of(source_ids, myself, devices, held)
    low = (myself - HALF) * src_count
    own_asked = named(own_src, low, SPAN * src_count).reshape(SPAN, src_count)
    own_ranks = ranks_of(own_asked)
    is_local = (jnp.arange(SPAN) == HALF)[:, None]
    own_place = jnp.where(is_local, jnp.arange(src_count, dtype=jnp.int32)[None, :], own_ranks)
    stage_of = jnp.array([STAGES.index(r - HALF) for r in range(SPAN)], jnp.int32)
    own_place = (own_place + 256 * stage_of[:, None]).reshape(-1)
    hits = (own_src - low)[:, None] == jnp.arange(SPAN * src_count, dtype=jnp.int32)[None, :]
    staged = jnp.sum(jnp.where(hits, own_place[None, :], 0), axis=1)
    stage, place = staged // 256, staged % 256

    own_tgt = rows_of(target_ids, myself, devices, held)
    low = (myself - HALF) * TB_DEV
    tgt_asked = named(own_tgt, low, SPAN * TB_DEV).reshape(SPAN, TB_DEV)
    tgt_place = ranks_of(tgt_asked) + CAP_T * jnp.arange(SPAN, dtype=jnp.int32)[:, None]
    hits = (own_tgt - low)[:, None] == jnp.arange(SPAN * TB_DEV, dtype=jnp.int32)[None, :]
    slot = jnp.sum(jnp.where(hits, tgt_place.reshape(-1)[None, :], 0), axis=1)

    index = jnp.arange(held, dtype=jnp.int32)
    key = stage * held + index
    position = jnp.sum((key[:, None] < key[None, :]).astype(jnp.int32), axis=0)
    item = (index * 256 + place) * 128 + slot
    packed = jnp.sum(jnp.where(position[None, :] == index[:, None], item[None, :], 0), axis=1)
    bounds = jnp.sum((stage[None, :] < jnp.arange(8)[:, None]).astype(jnp.int32), axis=1)

    box_asked = []
    for step in range(-HALF, HALF + 1):
        sender = myself - step
        valid = (sender >= 0) & (sender < devices)
        rows = rows_of(target_ids, sender, devices, held)
        box_asked.append(named(rows, myself * TB_DEV, TB_DEV) & valid)
    box_asked = jnp.stack(box_asked)
    places = jnp.where(box_asked, ranks_of(box_asked), -1).reshape(-1)

    acc = None
    for n in range(SPAN):
        src = source_field if n == 0 else arrived[n - 1]
        acc = stage_call(n, bounds, packed, weight_blocks, src, acc)
    boxes = [
        acc[step + HALF] if step == 0 else passed_along(acc[step + HALF], step)
        for step in range(-HALF, HALF + 1)
    ]
    return final_call(places, boxes)


def solution(mesh):
    return jax.shard_map(
        body,
        mesh=mesh,
        in_specs=(P(AXES, None, None), P(AXES, None, None), P(), P()),
        out_specs=P(AXES, None, None),
        check_vma=False,
    )
```
